8 devices in a mesh: dp: 1 (over z), tp: 8 (over x, y, core).
Axes of the slice: x: 2, y: 2, z: 1, core: 2. Of those that a mesh axis runs over, the one named last changes fastest.
Arguments:
- x: bfloat16 [2048, 2048], P('dp')
- dy: bfloat16 [2048, 2048], P('dp')
- gate: bfloat16 [2048, 6144], P('dp', 'tp')
- up: bfloat16 [2048, 6144], P('dp', 'tp')
- w_gate: bfloat16 [2048, 6144], P(None, 'tp')
- w_up: bfloat16 [2048, 6144], P(None, 'tp')
- w_down: bfloat16 [6144, 2048], P('tp')
Outputs:
- output 1: bfloat16 [2048, 2048], P('dp')
- output 2: bfloat16 [2048, 6144], P('dp', 'tp')
- output 3: bfloat16 [2048, 6144], P('dp', 'tp')
- output 4: bfloat16 [6144, 2048], P(('dp', 'tp'))
All inputs are finite; a program needn't handle non-finite values.
Results may differ from the reference program's by a relative error of at most 0.012.
Values are sent between devices in bfloat16 or wider.
A program may use at most 2 GiB of HBM per device.

```python
import jax
import jax.numpy as jnp

ROWS = 2048
D = 2048
FF = 6144


def act(gate, up):
    return jax.nn.silu(gate) * up


def setup_inputs(seed: int = 0, part: int = 0) -> dict:
    kx, ky, ka, kb, kg, ku, kd = jax.random.split(jax.random.key(seed), 7)
    kx, ky, ka, kb = (jax.random.fold_in(k, part) for k in (kx, ky, ka, kb))
    drawn = {
        "x": jax.random.normal(kx, (ROWS, D), jnp.float32),
        "dy": jax.random.normal(ky, (ROWS, D), jnp.float32),
        "gate": jax.random.normal(ka, (ROWS, FF), jnp.float32),
        "up": jax.random.normal(kb, (ROWS, FF), jnp.float32),
        "w_gate": jax.random.normal(kg, (D, FF), jnp.float32) * D**-0.5,
        "w_up": jax.random.normal(ku, (D, FF), jnp.float32) * D**-0.5,
        "w_down": jax.random.normal(kd, (FF, D), jnp.float32) * FF**-0.5,
    }
    return {k: v.astype(jnp.bfloat16) for k, v in drawn.items()}


def reference(x, dy, gate, up, w_gate, w_up, w_down):
    hidden, back = jax.vjp(act, gate.astype(jnp.float32), up.astype(jnp.float32))
    d_hidden = jnp.dot(dy, w_down.T, preferred_element_type=jnp.float32)
    d_gate, d_up = (g.astype(jnp.bfloat16) for g in back(d_hidden))
    dx = jnp.dot(d_gate, w_gate.T, preferred_element_type=jnp.float32) + jnp.dot(d_up, w_up.T, preferred_element_type=jnp.float32)
    dw_gate = jnp.dot(x.T, d_gate, preferred_element_type=jnp.float32)
    dw_up = jnp.dot(x.T, d_up, preferred_element_type=jnp.float32)
    dw_down = jnp.dot(hidden.astype(jnp.bfloat16).T, dy, preferred_element_type=jnp.float32)
    return tuple(g.astype(jnp.bfloat16) for g in (dx, dw_gate, dw_up, dw_down))
```

```python
import jax
import jax.numpy as jnp
from jax import lax
from jax.experimental import pallas as pl
from jax.experimental.pallas import tpu as pltpu
from jax.sharding import PartitionSpec as P

MESH = pl.DeviceIdType.MESH
BF, F32 = jnp.bfloat16, jnp.float32
NT = (((1,), (1,)), ((), ()))
TN = (((0,), (0,)), ((), ()))

ROWS, D, HID = 2048, 2048, 768
R = 256
C = ROWS // R
R2, R4 = R // 2, R // 4
OWN = D // 2
HC = OWN // 2
XB = 256
ACC, SS, XS = 4, 2, 3
LAG = 5

D2D, RS1, RS2, AG1, AG2, FIN = 0, 2, 4, 6, 8, 10
KINDS = 11


def dot(a, b, dims):
    return lax.dot_general(a, b, dims, preferred_element_type=F32)


def al(v, m):
    return pl.multiple_of(v, m)


def kernel(x, dy, gate, up, w_gate, w_up, w_down, dx, dwg, dwu, dwd,
           dyv, gv, uv, dg, du, hid, xv, acc, d2d_s, d2d_r, rs1_s, rs1_r, rs2_s, rs2_r,
           send, recv, lw, lc, lx):
    me = lax.axis_index("tp")
    c, y, xx = me % 2, (me // 2) % 2, me // 4
    partner = {"tp": me + 1 - 2 * c}
    ny = {"tp": me + 2 - 4 * y}
    nx = {"tp": me + 4 - 8 * xx}
    first, second = (xx, y), (y, xx)
    to_first, to_second = (nx, ny), (ny, nx)

    def load_chunk(k):
        slot = k % 2
        r = pl.ds(al(k * R, R), R)
        return [pltpu.make_async_copy(dy.at[r], dyv.at[r], lc.at[slot, 0]),
                pltpu.make_async_copy(gate.at[r], gv.at[slot], lc.at[slot, 1]),
                pltpu.make_async_copy(up.at[r], uv.at[slot], lc.at[slot, 2])]

    def load_x(j):
        slot = j % XS
        return pltpu.make_async_copy(x.at[:, pl.ds(al(j * XB, XB), XB)], xv.at[slot], lx.at[slot])

    def load_down(i):
        r = pl.ds(i * 256, 256)
        return pltpu.make_async_copy(w_down.at[r], dwd.at[r], lw.at[i])

    def wrows(own, h):
        return pl.ds(al((c if own else 1 - c) * OWN + h * HC, HC), HC)

    def load_w(own, h):
        r = wrows(own, h)
        i = 3 + 2 * (2 * own + h)
        return [pltpu.make_async_copy(w_gate.at[r], dwg.at[r], lw.at[i]),
                pltpu.make_async_copy(w_up.at[r], dwu.at[r], lw.at[i + 1])]

    def rc(src, dst, k, kind, dev):
        return pltpu.make_async_remote_copy(src, dst, send.at[k, kind], recv.at[k, kind],
                                            device_id=dev, device_id_type=MESH)

    def cols(h):
        return pl.ds(al(c * OWN + h * HC, HC), HC)

    def cp(k, kind, h=0):
        if kind == D2D:
            return rc(d2d_s.at[k % SS, h], d2d_r.at[k, h], k, kind + h, partner)
        if kind == RS1:
            return rc(rs1_s.at[k, h], rs1_r.at[k, h], k, kind + h, to_first[h])
        if kind == RS2:
            return rc(rs2_s.at[k, h], rs2_r.at[k, h], k, kind + h, to_second[h])
        if kind == AG1:
            b = dx.at[pl.ds(al(k * R + first[h] * R2 + second[h] * R4, R4), R4), cols(h)]
            return rc(b, b, k, kind + h, to_second[h])
        if kind == AG2:
            b = dx.at[pl.ds(al(k * R + first[h] * R2, R2), R2), cols(h)]
            return rc(b, b, k, kind + h, to_first[h])
        b = dx.at[pl.ds(al(k * R, R), R), pl.ds(al(c * OWN, OWN), OWN)]
        return rc(b, b, k, kind, partner)

    def hidden(k, i):
        r, n = pl.ds(al(k * R, R), R), slice(i * 256, (i + 1) * 256)
        slot = k % 2
        dh = dot(dyv[r, :], dwd[n, :], NT)
        g, u = gv[slot, :, n].astype(F32), uv[slot, :, n].astype(F32)
        s = jax.nn.sigmoid(g)
        silu = g * s
        hid[r, n] = (silu * u).astype(BF)
        du[r, n] = (dh * silu).astype(BF)
        dg[r, n] = (dh * u * (s + silu * (1.0 - s))).astype(BF)

    def term(k, own, h):
        r = pl.ds(al(k * R, R), R)
        w = wrows(own, h)
        t = dot(dg[r, :], dwg[w, :], NT) + dot(du[r, :], dwu[w, :], NT)
        if own:
            acc[k % ACC, h] = t
        else:
            d2d_s[k % SS, h] = t.astype(BF)

    def sum1(k):
        for h in range(2):
            cp(k, D2D, h).wait_recv()
        for h in range(2):
            keep, leave = (pl.ds(al(v * R2, R2), R2) for v in (first[h], 1 - first[h]))
            acc[k % ACC, h, keep] = acc[k % ACC, h, keep] + d2d_r[k, h, keep].astype(F32)
            rs1_s[k, h] = (acc[k % ACC, h, leave] + d2d_r[k, h, leave].astype(F32)).astype(BF)

    def sum2(k):
        for h in range(2):
            cp(k, RS1, h).wait_recv()
        for h in range(2):
            a, b = second[h], 1 - second[h]
            keep, leave = (pl.ds(al(first[h] * R2 + v * R4, R4), R4) for v in (a, b))
            rkeep, rleave = (pl.ds(al(v * R4, R4), R4) for v in (a, b))
            acc[k % ACC, h, keep] = acc[k % ACC, h, keep] + rs1_r[k, h, rkeep].astype(F32)
            rs2_s[k, h] = (acc[k % ACC, h, leave] + rs1_r[k, h, rleave].astype(F32)).astype(BF)

    def sum3(k):
        for h in range(2):
            cp(k, RS2, h).wait_recv()
        for h in range(2):
            p = first[h] * R2 + second[h] * R4
            dx[pl.ds(al(k * R + p, R4), R4), cols(h)] = (
                acc[k % ACC, h, pl.ds(al(p, R4), R4)] + rs2_r[k, h].astype(F32)).astype(BF)

    def go(k, kind):
        for h in range(2):
            cp(k, kind, h).start()

    def gather2(k):
        for h in range(2):
            cp(k, AG1, h).wait_recv()
        go(k, AG2)

    def gather3(k):
        for h in range(2):
            cp(k, AG2, h).wait_recv()
        cp(k, FIN).start()

    barrier = pltpu.get_barrier_semaphore()
    for dev in (partner, ny, nx):
        pl.semaphore_signal(barrier, inc=1, device_id=dev, device_id_type=MESH)

    zero = jnp.int32(0)
    load_down(0).start()
    for l in load_chunk(zero):
        l.start()
    load_down(1).start()
    load_down(2).start()

    def step(k, static):
        if static == 0:
            load_down(0).wait()
            for l in load_chunk(k):
                l.wait()
            for h in range(2):
                for l in load_w(0, h):
                    l.start()
            hidden(k, 0)
            load_down(1).wait()
            for h in range(2):
                for l in load_w(1, h):
                    l.start()
            hidden(k, 1)
            load_down(2).wait()
            for l in load_chunk(k + 1):
                l.start()
            hidden(k, 2)
        else:
            for l in load_chunk(k):
                l.wait()
            sum1(k - 1)
            hidden(k, 0)
            go(k - 1, RS1)
            if static is not None:
                for l in load_chunk(k + 1):
                    l.start()
            else:
                @pl.when(k + 1 < C)
                def _():
                    for l in load_chunk(k + 1):
                        l.start()
            hidden(k, 1)
            hidden(k, 2)
        for h in range(2):
            if static == 0:
                for l in load_w(0, h):
                    l.wait()
                if h == 0:
                    pl.semaphore_wait(barrier, 3)
            if static is None or static >= SS:
                cp(k - SS, D2D, h).wait_send()
            term(k, 0, h)
            cp(k, D2D, h).start()
        if static == 0:
            for h in range(2):
                for l in load_w(1, h):
                    l.wait()
        if static is None or static >= 2:
            sum2(k - 2)
        term(k, 1, 0)
        if static is None or static >= 2:
            go(k - 2, RS2)
        if static is None or static >= 3:
            sum3(k - 3)
        term(k, 1, 1)
        if static is None:
            @pl.when(k >= LAG)
            def _():
                go(k - LAG, AG1)

    for k in range(3):
        step(jnp.int32(k), k)
        if k == 1:
            for j in range(XS):
                load_x(jnp.int32(j)).start()

    @pl.loop(3, C)
    def _(k):
        step(k, None)

    def wg(j, out, d):
        out[pl.ds(al(j * XB, XB), XB), :] = dot(xv[j % XS], d[...], TN).astype(BF)

    def wd(j):
        n = pl.ds(al(j * XB, XB), XB)
        dwd[:, n] = dot(hid[...], dyv[:, n], TN).astype(BF)

    i32 = jnp.int32
    j = i32(0)
    load_x(j).wait()
    sum1(i32(C - 1))
    wg(j, dwg, dg)
    go(i32(C - 1), RS1)
    gather2(i32(0))
    sum2(i32(C - 2))
    wg(j, dwu, du)
    go(i32(C - 2), RS2)
    load_x(j + XS).start()
    go(i32(C - LAG), AG1)
    sum3(i32(C - 3))
    wd(j)
    go(i32(C - LAG + 1), AG1)
    gather2(i32(1))
    j = i32(1)
    load_x(j).wait()
    sum2(i32(C - 1))
    wg(j, dwg, dg)
    go(i32(C - 1), RS2)
    sum3(i32(C - 2))
    wg(j, dwu, du)
    load_x(j + XS).start()
    go(i32(C - LAG + 2), AG1)
    gather2(i32(2))
    wd(j)
    j = i32(2)
    load_x(j).wait()
    sum3(i32(C - 1))
    wg(j, dwg, dg)
    go(i32(C - LAG + 3), AG1)
    go(i32(C - LAG + 4), AG1)
    gather2(i32(3))
    wg(j, dwu, du)
    load_x(j + XS).start()
    gather3(i32(0))
    wd(j)

    @pl.loop(3, C)
    def _(j):
        load_x(j).wait()
        wg(j, dwg, dg)

        @pl.when(j + 1 < C)
        def _():
            gather2(j + 1)

        wg(j, dwu, du)

        @pl.when(j + XS < C)
        def _():
            load_x(j + XS).start()

        gather3(j - 2)
        wd(j)

    gather3(i32(C - 2))
    gather3(i32(C - 1))

    @pl.loop(0, C)
    def _(k):
        @pl.when(k >= C - SS)
        def _():
            for h in range(2):
                cp(k, D2D, h).wait_send()

        for kind in (RS1, RS2, AG1, AG2):
            for h in range(2):
                cp(k, kind, h).wait_send()
        cp(k, FIN).wait()


def put(*refs):
    n = len(refs) // 2
    sem = refs[-1]
    copies = [pltpu.make_async_copy(refs[i], refs[n + i], sem.at[i]) for i in range(n)]
    for cpy in copies:
        cpy.start()
    for cpy in copies:
        cpy.wait()


def solution(mesh):
    shapes = [(ROWS, D), (D, HID), (D, HID), (HID, D)]

    def step(*args):
        outs = pl.pallas_call(
            kernel,
            out_shape=[pltpu.VMEM(s, BF) for s in shapes],
            in_specs=[pl.BlockSpec(memory_space=pltpu.HBM)] * 7,
            out_specs=[pl.BlockSpec(memory_space=pltpu.VMEM)] * 4,
            scratch_shapes=[
                pltpu.VMEM((ROWS, D), BF),
                pltpu.VMEM((2, R, HID), BF),
                pltpu.VMEM((2, R, HID), BF),
                pltpu.VMEM((ROWS, HID), BF),
                pltpu.VMEM((ROWS, HID), BF),
                pltpu.VMEM((ROWS, HID), BF),
                pltpu.VMEM((XS, ROWS, XB), BF),
                pltpu.VMEM((ACC, 2, R, HC), F32),
                pltpu.VMEM((SS, 2, R, HC), BF),
                pltpu.VMEM((C, 2, R, HC), BF),
                pltpu.VMEM((C, 2, R2, HC), BF),
                pltpu.VMEM((C, 2, R2, HC), BF),
                pltpu.VMEM((C, 2, R4, HC), BF),
                pltpu.VMEM((C, 2, R4, HC), BF),
                pltpu.SemaphoreType.DMA((C, KINDS)),
                pltpu.SemaphoreType.DMA((C, KINDS)),
                pltpu.SemaphoreType.DMA((11,)),
                pltpu.SemaphoreType.DMA((2, 3)),
                pltpu.SemaphoreType.DMA((XS,)),
            ],
            compiler_params=pltpu.CompilerParams(collective_id=0, has_side_effects=True, vmem_limit_bytes=45 * 2**20),
        )(*args)
        return tuple(pl.pallas_call(
            put,
            out_shape=[pltpu.HBM(s, BF) for s in shapes],
            in_specs=[pl.BlockSpec(memory_space=pltpu.VMEM)] * 4,
            out_specs=[pl.BlockSpec(memory_space=pltpu.HBM)] * 4,
            scratch_shapes=[pltpu.SemaphoreType.DMA((4,))],
            compiler_params=pltpu.CompilerParams(vmem_limit_bytes=2**20),
        )(*outs))

    tokens, columns, rows = P("dp", None), P(None, "tp"), P("tp", None)
    return jax.shard_map(
        step,
        mesh=mesh,
        in_specs=(tokens, tokens, P("dp", "tp"), P("dp", "tp"), columns, columns, rows),
        out_specs=(tokens, P("dp", "tp"), P("dp", "tp"), P(("dp", "tp"), None)),
        check_vma=False,
    )
```

```python
import jax
import jax.numpy as jnp
from jax import lax
from jax.experimental import pallas as pl
from jax.experimental.pallas import tpu as pltpu
from jax.sharding import PartitionSpec as P

MESH = pl.DeviceIdType.MESH
BF, F32 = jnp.bfloat16, jnp.float32
NT = (((1,), (1,)), ((), ()))
TN = (((0,), (0,)), ((), ()))

ROWS, D, HID = 2048, 2048, 768
R = 256
C = ROWS // R
R2, R4 = R // 2, R // 4
OWN = D // 2
HC = OWN // 2
XB = 256
DB = 512
SS, XS, S1, S2, S3 = 2, 3, 2, 3, 3

D2D, RS1, RS2, AG1, AG2, FIN1, FIN2 = 0, 2, 4, 6, 8, 10, 12
KINDS = 14


def dot(a, b, dims):
    return lax.dot_general(a, b, dims, preferred_element_type=F32)


def al(v, m):
    return pl.multiple_of(v, m)


def kernel(x, dy, gate, up, w_gate, w_up, w_down, dx, dw, dwd,
           dyv, gv, uv, dgu, hid, xv, acc1, acc2, acc3, d2d_s, d2d_r, rs1_s, rs1_r, rs2_s, rs2_r,
           send, recv, lw, lc, lx):
    me = lax.axis_index("tp")
    c, y, xx = me % 2, (me // 2) % 2, me // 4
    partner = {"tp": me + 1 - 2 * c}
    ny = {"tp": me + 2 - 4 * y}
    nx = {"tp": me + 4 - 8 * xx}
    first, second = (xx, y), (y, xx)
    to_first, to_second = (nx, ny), (ny, nx)
    both = (0, 1)
    i32 = jnp.int32

    def load_chunk(k):
        slot = k % 2
        r = pl.ds(al(k * R, R), R)
        return [pltpu.make_async_copy(dy.at[r], dyv.at[r], lc.at[slot, 0]),
                pltpu.make_async_copy(gate.at[r], gv.at[slot], lc.at[slot, 1]),
                pltpu.make_async_copy(up.at[r], uv.at[slot], lc.at[slot, 2])]

    def load_x(j):
        slot = j % XS
        return pltpu.make_async_copy(x.at[:, pl.ds(j * XB, XB)], xv.at[slot], lx.at[slot])

    def load_down(i):
        r = pl.ds(i * 256, 256)
        return pltpu.make_async_copy(w_down.at[r], dwd.at[r], lw.at[i])

    def wrows(own):
        return pl.ds(al((c if own else 1 - c) * OWN, OWN), OWN)

    def load_w(own):
        r = wrows(own)
        return [pltpu.make_async_copy(w_gate.at[r], dw.at[r, pl.ds(0, HID)], lw.at[3 + 2 * own]),
                pltpu.make_async_copy(w_up.at[r], dw.at[r, pl.ds(HID, HID)], lw.at[4 + 2 * own])]

    def start(copies):
        for l in copies:
            l.start()

    def wait(copies):
        for l in copies:
            l.wait()

    def rc(src, dst, k, kind, dev):
        return pltpu.make_async_remote_copy(src, dst, send.at[k, kind], recv.at[k, kind],
                                            device_id=dev, device_id_type=MESH)

    def cols(h):
        return pl.ds(al(c * OWN + h * HC, HC), HC)

    def cp(k, kind, h):
        if kind == D2D:
            return rc(d2d_s.at[k % SS, h], d2d_r.at[k, h], k, kind + h, partner)
        if kind == RS1:
            return rc(rs1_s.at[k, h], rs1_r.at[k, h], k, kind + h, to_first[h])
        if kind == RS2:
            return rc(rs2_s.at[k, h], rs2_r.at[k, h], k, kind + h, to_second[h])
        if kind == AG1:
            b = dx.at[pl.ds(al(k * R + first[h] * R2 + second[h] * R4, R4), R4), cols(h)]
            return rc(b, b, k, kind + h, to_second[h])
        p = (1 - first[h]) if kind == FIN2 else first[h]
        b = dx.at[pl.ds(al(k * R + p * R2, R2), R2), cols(h)]
        return rc(b, b, k, kind + h, to_first[h] if kind == AG2 else partner)

    def go(k, kind, halves=both):
        for h in halves:
            cp(k, kind, h).start()

    def arrived(k, kind, halves=both):
        for h in halves:
            cp(k, kind, h).wait_recv()

    def hidden(k, i):
        r, n = pl.ds(al(k * R, R), R), slice(i * 256, (i + 1) * 256)
        slot = k % 2
        dh = dot(dyv[r, :], dwd[n, :], NT)
        g, u = gv[slot, :, n].astype(F32), uv[slot, :, n].astype(F32)
        s = jax.nn.sigmoid(g)
        silu = g * s
        hid[r, n] = (silu * u).astype(BF)
        dgu[r, HID + i * 256:HID + (i + 1) * 256] = (dh * silu).astype(BF)
        dgu[r, n] = (dh * u * (s + silu * (1.0 - s))).astype(BF)

    def term(k, own, halves=both):
        r = pl.ds(al(k * R, R), R)
        for h in halves:
            w = pl.ds(al((c if own else 1 - c) * OWN + h * HC, HC), HC)
            t = dot(dgu[r, :], dw[w, :], NT)
            if own:
                acc1[k % S1, h] = t
            else:
                d2d_s[k % SS, h] = t.astype(BF)

    def sum1(k, halves=both):
        arrived(k, D2D, halves)
        for h in halves:
            keep, leave = (pl.ds(al(v * R2, R2), R2) for v in (first[h], 1 - first[h]))
            rs1_s[k, h] = (acc1[k % S1, h, leave] + d2d_r[k, h, leave].astype(F32)).astype(BF)
            acc2[k % S2, h] = acc1[k % S1, h, keep] + d2d_r[k, h, keep].astype(F32)
        go(k, RS1, halves)

    def sum2(k):
        arrived(k, RS1)
        for h in both:
            keep, leave = (pl.ds(al(v * R4, R4), R4) for v in (second[h], 1 - second[h]))
            rs2_s[k, h] = (acc2[k % S2, h, leave] + rs1_r[k, h, leave].astype(F32)).astype(BF)
            acc3[k % S3, h] = acc2[k % S2, h, keep] + rs1_r[k, h, keep].astype(F32)
        go(k, RS2)

    def sum3(k):
        arrived(k, RS2)
        for h in both:
            p = first[h] * R2 + second[h] * R4
            dx[pl.ds(al(k * R + p, R4), R4), cols(h)] = (acc3[k % S3, h] + rs2_r[k, h].astype(F32)).astype(BF)
        go(k, AG1)

    def gather2(k):
        arrived(k, AG1)
        go(k, AG2)
        go(k, FIN1)

    def gather3(k):
        arrived(k, AG2)
        go(k, FIN2)

    barrier = pltpu.get_barrier_semaphore()
    for dev in (partner, ny, nx):
        pl.semaphore_signal(barrier, inc=1, device_id=dev, device_id_type=MESH)

    k0 = i32(0)
    load_down(0).start()
    start(load_chunk(k0))
    load_down(1).start()
    load_down(2).start()
    load_down(0).wait()
    wait(load_chunk(k0))
    start(load_w(0))
    load_down(1).wait()
    load_down(2).wait()
    start(load_w(1))
    for i in range(3):
        hidden(k0, i)
    start(load_chunk(i32(1)))
    wait(load_w(0))
    pl.semaphore_wait(barrier, 3)
    for h in both:
        term(k0, 0, (h,))
        go(k0, D2D, (h,))
    wait(load_w(1))
    for h in both:
        term(k0, 1, (h,))
        sum1(k0, (h,))
    for j in range(XS):
        load_x(j).start()

    @pl.loop(1, C)
    def _(k):
        @pl.when(k >= 3)
        def _():
            sum2(k - 3)

        @pl.when(k >= 5)
        def _():
            sum3(k - 5)

        wait(load_chunk(k))

        @pl.when(k + 1 < C)
        def _():
            start(load_chunk(k + 1))

        for i in range(3):
            hidden(k, i)

        @pl.when(k >= 2)
        def _():
            sum1(k - 1)
            for h in both:
                cp(k - 2, D2D, h).wait_send()

        term(k, 0)
        go(k, D2D)
        term(k, 1)

    def piece_x(j):
        load_x(j).wait()
        dw[j * XB:(j + 1) * XB, :] = dot(xv[j % XS], dgu[...], TN).astype(BF)
        if j + XS < D // XB:
            load_x(j + XS).start()

    def piece_y(j):
        n = slice(j * DB, (j + 1) * DB)
        dwd[:, n] = dot(hid[...], dyv[:, n], TN).astype(BF)

    pieces = []
    for j in range(4):
        pieces += [lambda j=j: piece_x(2 * j), lambda j=j: piece_x(2 * j + 1), lambda j=j: piece_y(j)]
    events = {
        0: [(sum1, 7)],
        1: [(sum2, 5)],
        2: [(sum3, 3)],
        3: [(sum2, 6), (gather2, 0)],
        4: [(sum3, 4), (gather2, 1)],
        5: [(sum2, 7), (sum3, 5), (gather2, 2)],
        6: [(sum3, 6), (gather2, 3)],
        7: [(sum3, 7)],
        8: [(gather2, 4)],
        9: [(gather2, 5), (gather3, 0)],
        10: [(gather2, 6), (gather3, 1)],
        11: [(gather2, 7), (gather3, 2)],
    }
    for i, piece in enumerate(pieces):
        for f, k in events[i]:
            f(i32(k))
        piece()
    for k in range(3, C):
        gather3(i32(k))

    @pl.loop(0, C)
    def _(k):
        @pl.when(k >= C - SS)
        def _():
            for h in both:
                cp(k, D2D, h).wait_send()

        for h in both:
            for kind in (RS1, RS2, AG1, AG2):
                cp(k, kind, h).wait_send()
            for kind in (FIN1, FIN2):
                cp(k, kind, h).wait()


def put(dx, dw, dwd, o_dx, o_gate, o_up, o_down, sem):
    copies = [pltpu.make_async_copy(dx, o_dx, sem.at[0]),
              pltpu.make_async_copy(dw.at[:, pl.ds(0, HID)], o_gate, sem.at[1]),
              pltpu.make_async_copy(dw.at[:, pl.ds(HID, HID)], o_up, sem.at[2]),
              pltpu.make_async_copy(dwd, o_down, sem.at[3])]
    for c in copies:
        c.start()
    for c in copies:
        c.wait()


def solution(mesh):
    def step(*args):
        outs = pl.pallas_call(
            kernel,
            out_shape=[pltpu.VMEM((ROWS, D), BF), pltpu.VMEM((D, 2 * HID), BF), pltpu.VMEM((HID, D), BF)],
            in_specs=[pl.BlockSpec(memory_space=pltpu.HBM)] * 7,
            out_specs=[pl.BlockSpec(memory_space=pltpu.VMEM)] * 3,
            scratch_shapes=[
                pltpu.VMEM((ROWS, D), BF),
                pltpu.VMEM((2, R, HID), BF),
                pltpu.VMEM((2, R, HID), BF),
                pltpu.VMEM((ROWS, 2 * HID), BF),
                pltpu.VMEM((ROWS, HID), BF),
                pltpu.VMEM((XS, ROWS, XB), BF),
                pltpu.VMEM((S1, 2, R, HC), F32),
                pltpu.VMEM((S2, 2, R2, HC), F32),
                pltpu.VMEM((S3, 2, R4, HC), F32),
                pltpu.VMEM((SS, 2, R, HC), BF),
                pltpu.VMEM((C, 2, R, HC), BF),
                pltpu.VMEM((C, 2, R2, HC), BF),
                pltpu.VMEM((C, 2, R2, HC), BF),
                pltpu.VMEM((C, 2, R4, HC), BF),
                pltpu.VMEM((C, 2, R4, HC), BF),
                pltpu.SemaphoreType.DMA((C, KINDS)),
                pltpu.SemaphoreType.DMA((C, KINDS)),
                pltpu.SemaphoreType.DMA((7,)),
                pltpu.SemaphoreType.DMA((2, 3)),
                pltpu.SemaphoreType.DMA((XS,)),
            ],
            compiler_params=pltpu.CompilerParams(collective_id=0, has_side_effects=True, vmem_limit_bytes=45 * 2**20),
        )(*args)
        shapes = [(ROWS, D), (D, HID), (D, HID), (HID, D)]
        return tuple(pl.pallas_call(
            put,
            out_shape=[pltpu.HBM(s, BF) for s in shapes],
            in_specs=[pl.BlockSpec(memory_space=pltpu.VMEM)] * 3,
            out_specs=[pl.BlockSpec(memory_space=pltpu.HBM)] * 4,
            scratch_shapes=[pltpu.SemaphoreType.DMA((4,))],
            compiler_params=pltpu.CompilerParams(vmem_limit_bytes=2**20),
        )(*outs))

    tokens, columns, rows = P("dp", None), P(None, "tp"), P("tp", None)
    return jax.shard_map(
        step,
        mesh=mesh,
        in_specs=(tokens, tokens, P("dp", "tp"), P("dp", "tp"), columns, columns, rows),
        out_specs=(tokens, P("dp", "tp"), P("dp", "tp"), P(("dp", "tp"), None)),
        check_vma=False,
    )
```

```python
import jax
import jax.numpy as jnp
from jax import lax
from jax.experimental import pallas as pl
from jax.experimental.pallas import tpu as pltpu
from jax.sharding import PartitionSpec as P

MESH = pl.DeviceIdType.MESH
BF, F32 = jnp.bfloat16, jnp.float32
NT = (((1,), (1,)), ((), ()))
TN = (((0,), (0,)), ((), ()))

ROWS, D, HID = 2048, 2048, 768
R = 256
C = ROWS // R
R2, R4 = R // 2, R // 4
OWN = D // 2
HC = OWN // 2
XB = 256
DB = 512
SS, XS, S1, S2, S3 = 2, 3, 2, 3, 3

D2D, RS1, RS2, AG1, AG2, FIN1, FIN2 = range(7)


def dot(a, b, dims):
    return lax.dot_general(a, b, dims, preferred_element_type=F32)


def al(v, m):
    return pl.multiple_of(v, m)


def kernel(x, dy, gate, up, w_gate, w_up, w_down, dx, dw, dwd,
           dyv, gv, uv, dgu, hid, st0, st1, xv, acc1, acc2, acc3, d2d_s, d2d_r, rs1_s, rs1_r, rs2_s, rs2_r,
           send, recv, fin, lw, lc, lx):
    me = lax.axis_index("tp")
    c, y, xx = me % 2, (me // 2) % 2, me // 4
    partner = {"tp": me + 1 - 2 * c}
    ny = {"tp": me + 2 - 4 * y}
    nx = {"tp": me + 4 - 8 * xx}
    first, second = (xx, y), (y, xx)
    to_first, to_second = (nx, ny), (ny, nx)
    both = (0, 1)
    i32 = jnp.int32

    def load_chunk(k):
        slot = k % 2
        r = pl.ds(al(k * R, R), R)
        return [pltpu.make_async_copy(dy.at[r], dyv.at[r], lc.at[slot, 0]),
                pltpu.make_async_copy(gate.at[r], gv.at[slot], lc.at[slot, 1]),
                pltpu.make_async_copy(up.at[r], uv.at[slot], lc.at[slot, 2])]

    def load_x(j):
        slot = j % XS
        return pltpu.make_async_copy(x.at[:, pl.ds(j * XB, XB)], xv.at[slot], lx.at[slot])

    def load_down(i):
        r = pl.ds(i * 256, 256)
        return pltpu.make_async_copy(w_down.at[r], dwd.at[r], lw.at[i])

    def wrows(own):
        return pl.ds(al((c if own else 1 - c) * OWN, OWN), OWN)

    def load_w(own):
        r = wrows(own)
        return [pltpu.make_async_copy(w_gate.at[r], dw.at[r, pl.ds(0, HID)], lw.at[3 + 2 * own]),
                pltpu.make_async_copy(w_up.at[r], dw.at[r, pl.ds(HID, HID)], lw.at[4 + 2 * own])]

    def start(copies):
        for l in copies:
            l.start()

    def wait(copies):
        for l in copies:
            l.wait()

    def rc(src, dst, kind, sem, dev, slot=0):
        return pltpu.make_async_remote_copy(src, dst, send.at[7 + slot if kind == D2D else kind], sem,
                                            device_id=dev, device_id_type=MESH)

    def cols(h):
        return pl.ds(al(c * OWN + h * HC, HC), HC)

    def cp(k, kind, h, first_chunk=False):
        sem = fin.at[kind - FIN1] if kind >= FIN1 else recv.at[C if first_chunk and h else k, kind]
        if kind == D2D:
            return rc(d2d_s.at[k % SS, h], d2d_r.at[k, h], kind, sem, partner, k % SS)
        if kind == RS1:
            return rc(rs1_s.at[k, h], rs1_r.at[k, h], kind, sem, to_first[h])
        if kind == RS2:
            return rc(rs2_s.at[k, h], rs2_r.at[k, h], kind, sem, to_second[h])
        if kind == AG1:
            b = dx.at[pl.ds(al(k * R + first[h] * R2 + second[h] * R4, R4), R4), cols(h)]
            return rc(b, b, kind, sem, to_second[h])
        p = (1 - first[h]) if kind == FIN2 else first[h]
        b = dx.at[pl.ds(al(k * R + p * R2, R2), R2), cols(h)]
        return rc(b, b, kind, sem, to_first[h] if kind == AG2 else partner)

    def go(k, kind):
        for h in both:
            cp(k, kind, h).start()

    sizes = {D2D: d2d_r, RS1: rs1_r, RS2: rs2_r, AG1: rs2_r, AG2: rs1_r, FIN1: rs1_r, FIN2: rs1_r}

    def sent(slot):
        rc(d2d_s.at[slot], d2d_r.at[0], D2D, fin.at[0], partner, slot).wait_send()

    def arrived(k, kind):
        b = sizes[kind].at[k]
        rc(b, b, kind, recv.at[k, kind], partner).wait_recv()

    stage = (st0, st1)

    def hidden(k, slot):
        r = pl.ds(al(k * R, R), R)
        st = stage[slot]
        dh = dot(dyv[r, :], dwd[...], NT)
        for i in range(3):
            n = slice(i * 256, (i + 1) * 256)
            g, u, d = gv[slot, :, n].astype(F32), uv[slot, :, n].astype(F32), dh[:, n]
            s = jax.nn.sigmoid(g)
            silu = g * s
            hid[r, n] = (silu * u).astype(BF)
            m = slice(HID + i * 256, HID + (i + 1) * 256)
            d_up = (d * silu).astype(BF)
            d_gate = (d * u * (s + silu * (1.0 - s))).astype(BF)
            st[:, m], dgu[r, m] = d_up, d_up
            st[:, n], dgu[r, n] = d_gate, d_gate

    def term(k, slot, own, halves=both):
        n = HC * len(halves)
        w = pl.ds(al((c if own else 1 - c) * OWN + halves[0] * HC, HC), n)
        t = dot(stage[slot][...], dw[w, :], NT)
        for h in halves:
            part = t[:, (h - halves[0]) * HC:(h - halves[0] + 1) * HC]
            if own:
                acc1[slot, h] = part
            else:
                d2d_s[slot, h] = part.astype(BF)

    def add1(k, h):
        keep, leave = (pl.ds(al(v * R2, R2), R2) for v in (first[h], 1 - first[h]))
        rs1_s[k, h] = (acc1[k % S1, h, leave] + d2d_r[k, h, leave].astype(F32)).astype(BF)
        acc2[k % S2, h] = acc1[k % S1, h, keep] + d2d_r[k, h, keep].astype(F32)

    def sum1(k):
        arrived(k, D2D)
        for h in both:
            add1(k, h)
        go(k, RS1)

    def sum2(k):
        arrived(k, RS1)
        for h in both:
            keep, leave = (pl.ds(al(v * R4, R4), R4) for v in (second[h], 1 - second[h]))
            rs2_s[k, h] = (acc2[k % S2, h, leave] + rs1_r[k, h, leave].astype(F32)).astype(BF)
            acc3[k % S3, h] = acc2[k % S2, h, keep] + rs1_r[k, h, keep].astype(F32)
        go(k, RS2)

    def sum3(k):
        arrived(k, RS2)
        for h in both:
            p = first[h] * R2 + second[h] * R4
            dx[pl.ds(al(k * R + p, R4), R4), cols(h)] = (acc3[k % S3, h] + rs2_r[k, h].astype(F32)).astype(BF)
        go(k, AG1)

    def gather2(k):
        arrived(k, AG1)
        go(k, AG2)
        go(k, FIN1)

    def gather3(k):
        arrived(k, AG2)
        go(k, FIN2)

    barrier = pltpu.get_barrier_semaphore()
    for dev in (partner, ny, nx):
        pl.semaphore_signal(barrier, inc=1, device_id=dev, device_id_type=MESH)

    k0 = i32(0)
    chunk0 = load_chunk(k0)
    for i in range(3):
        load_down(i).start()
        chunk0[i].start()
    start(load_w(0))
    start(load_w(1))
    start(load_chunk(i32(1)))
    for i in range(3):
        load_down(i).wait()
    wait(chunk0)
    hidden(k0, 0)
    wait(load_w(0))
    pl.semaphore_wait(barrier, 3)
    term(k0, 0, 0)
    for h in both:
        cp(k0, D2D, h, True).start()
    wait(load_w(1))
    wait(load_chunk(i32(1)))
    start(load_chunk(i32(2)))
    hidden(i32(1), 1)
    term(k0, 0, 1)
    for h in both:
        cp(k0, D2D, h, True).wait_recv()
        add1(k0, h)
        cp(k0, RS1, h).start()
    for j in range(XS):
        load_x(j).start()

    def step(k, slot, last=False):
        if not last:
            @pl.when(k + 2 < C)
            def _():
                start(load_chunk(k + 2))

        @pl.when(k >= 2)
        def _():
            sum1(k - 1)

        @pl.when(k >= 4)
        def _():
            sum2(k - 3)

        @pl.when(k >= 5)
        def _():
            sum3(k - 5)

        @pl.when(k >= 2)
        def _():
            sent(slot)

        term(k, slot, 0)
        go(k, D2D)
        if slot == 0:
            @pl.when(k == 2)
            def _():
                sum2(i32(0))

        if not last:
            wait(load_chunk(k + 1))
            hidden(k + 1, 1 - slot)
        term(k, slot, 1)

    @pl.loop(0, C // 2 - 1)
    def _(i):
        step(2 * i + 1, 1)
        step(2 * i + 2, 0)

    step(i32(C - 1), 1, last=True)

    def piece_x(j):
        load_x(j).wait()
        dw[j * XB:(j + 1) * XB, :] = dot(xv[j % XS], dgu[...], TN).astype(BF)
        if j + XS < D // XB:
            load_x(j + XS).start()

    def piece_y(j):
        n = slice(j * DB, (j + 1) * DB)
        dwd[:, n] = dot(hid[...], dyv[:, n], TN).astype(BF)

    pieces = []
    for j in range(4):
        pieces += [lambda j=j: piece_x(2 * j), lambda j=j: piece_x(2 * j + 1), lambda j=j: piece_y(j)]
    events = {
        0: [(sum1, 7)],
        1: [(sum2, 5)],
        2: [(sum3, 3)],
        3: [(sum2, 6)],
        4: [(sum3, 4), (gather2, 0)],
        5: [(gather2, 1)],
        6: [(sum2, 7), (gather2, 2)],
        7: [(sum3, 5)],
        8: [(sum3, 6), (gather2, 3)],
        9: [(gather2, 4), (gather3, 0)],
        10: [(sum3, 7)],
        11: [(gather2, 5), (gather3, 1)],
    }
    for i, piece in enumerate(pieces):
        for f, k in events[i]:
            f(i32(k))
        piece()
    for f, k in [(gather2, 6), (gather3, 2), (gather3, 3), (gather3, 4), (gather2, 7), (gather3, 5), (gather3, 6), (gather3, 7)]:
        f(i32(k))

    for kind, b in sizes.items():
        w = rc(b, b, kind, fin.at[max(kind - FIN1, 0)], partner)
        if kind >= FIN1:
            w.wait_recv()
        if kind != D2D:
            w.wait_send()
    for slot in range(SS):
        sent(slot)


def put(dx, dw, dwd, o_dx, o_gate, o_up, o_down, sem):
    copies = [pltpu.make_async_copy(dx, o_dx, sem.at[0]),
              pltpu.make_async_copy(dw.at[:, pl.ds(0, HID)], o_gate, sem.at[1]),
              pltpu.make_async_copy(dw.at[:, pl.ds(HID, HID)], o_up, sem.at[2]),
              pltpu.make_async_copy(dwd, o_down, sem.at[3])]
    for c in copies:
        c.start()
    for c in copies:
        c.wait()


def solution(mesh):
    def step(*args):
        outs = pl.pallas_call(
            kernel,
            out_shape=[pltpu.VMEM((ROWS, D), BF), pltpu.VMEM((D, 2 * HID), BF), pltpu.VMEM((HID, D), BF)],
            in_specs=[pl.BlockSpec(memory_space=pltpu.HBM)] * 7,
            out_specs=[pl.BlockSpec(memory_space=pltpu.VMEM)] * 3,
            scratch_shapes=[
                pltpu.VMEM((ROWS, D), BF),
                pltpu.VMEM((2, R, HID), BF),
                pltpu.VMEM((2, R, HID), BF),
                pltpu.VMEM((ROWS, 2 * HID), BF),
                pltpu.VMEM((ROWS, HID), BF),
                pltpu.VMEM((R, 2 * HID), BF),
                pltpu.VMEM((R, 2 * HID), BF),
                pltpu.VMEM((XS, ROWS, XB), BF),
                pltpu.VMEM((S1, 2, R, HC), F32),
                pltpu.VMEM((S2, 2, R2, HC), F32),
                pltpu.VMEM((S3, 2, R4, HC), F32),
                pltpu.VMEM((SS, 2, R, HC), BF),
                pltpu.VMEM((C, 2, R, HC), BF),
                pltpu.VMEM((C, 2, R2, HC), BF),
                pltpu.VMEM((C, 2, R2, HC), BF),
                pltpu.VMEM((C, 2, R4, HC), BF),
                pltpu.VMEM((C, 2, R4, HC), BF),
                pltpu.SemaphoreType.DMA((7 + SS,)),
                pltpu.SemaphoreType.DMA((C + 1, 5)),
                pltpu.SemaphoreType.DMA((2,)),
                pltpu.SemaphoreType.DMA((7,)),
                pltpu.SemaphoreType.DMA((2, 3)),
                pltpu.SemaphoreType.DMA((XS,)),
            ],
            compiler_params=pltpu.CompilerParams(collective_id=0, has_side_effects=True, vmem_limit_bytes=46 * 2**20),
        )(*args)
        shapes = [(ROWS, D), (D, HID), (D, HID), (HID, D)]
        return tuple(pl.pallas_call(
            put,
            out_shape=[pltpu.HBM(s, BF) for s in shapes],
            in_specs=[pl.BlockSpec(memory_space=pltpu.VMEM)] * 3,
            out_specs=[pl.BlockSpec(memory_space=pltpu.HBM)] * 4,
            scratch_shapes=[pltpu.SemaphoreType.DMA((4,))],
            compiler_params=pltpu.CompilerParams(vmem_limit_bytes=2**20),
        )(*outs))

    tokens, columns, rows = P("dp", None), P(None, "tp"), P("tp", None)
    return jax.shard_map(
        step,
        mesh=mesh,
        in_specs=(tokens, tokens, P("dp", "tp"), P("dp", "tp"), columns, columns, rows),
        out_specs=(tokens, P("dp", "tp"), P("dp", "tp"), P(("dp", "tp"), None)),
        check_vma=False,
    )
```

```python
import jax
import jax.numpy as jnp
from jax import lax
from jax.experimental import pallas as pl
from jax.experimental.pallas import tpu as pltpu
from jax.sharding import PartitionSpec as P

MESH = pl.DeviceIdType.MESH
BF, F32 = jnp.bfloat16, jnp.float32
NT = (((1,), (1,)), ((), ()))
TN = (((0,), (0,)), ((), ()))

ROWS, D, HID = 2048, 2048, 768
R = 256
C = ROWS // R
R2, R4 = R // 2, R // 4
OWN = D // 2
HC = OWN // 2
XB = 256
DB = 512
SS, XS, S1, S2, S3 = 2, 3, 2, 3, 3

D2D, RS1, RS2, AG1, AG2, FIN1, FIN2 = range(7)


def dot(a, b, dims):
    return lax.dot_general(a, b, dims, preferred_element_type=F32)


def al(v, m):
    return pl.multiple_of(v, m)


def kernel(x, dy, gate, up, w_gate, w_up, w_down, dx, dw, dwd,
           dyv, gv, uv, dgu, hid, st0, st1, xv, acc1, acc2, acc3, d2d_s, d2d_r, rs1_s, rs1_r, rs2_s, rs2_r,
           send, recv, fin, lw, lc, lx):
    me = lax.axis_index("tp")
    c, y, xx = me % 2, (me // 2) % 2, me // 4
    partner = {"tp": me + 1 - 2 * c}
    ny = {"tp": me + 2 - 4 * y}
    nx = {"tp": me + 4 - 8 * xx}
    first, second = (xx, y), (y, xx)
    to_first, to_second = (nx, ny), (ny, nx)
    both = (0, 1)
    i32 = jnp.int32

    def load_chunk(k):
        slot = k % 2
        r = pl.ds(al(k * R, R), R)
        return [pltpu.make_async_copy(dy.at[r], dyv.at[r], lc.at[slot, 0]),
                pltpu.make_async_copy(gate.at[r], gv.at[slot], lc.at[slot, 1]),
                pltpu.make_async_copy(up.at[r], uv.at[slot], lc.at[slot, 2])]

    def load_x(j):
        slot = j % XS
        return pltpu.make_async_copy(x.at[:, pl.ds(j * XB, XB)], xv.at[slot], lx.at[slot])

    def load_down(i):
        r = pl.ds(i * 256, 256)
        return pltpu.make_async_copy(w_down.at[r], dwd.at[r], lw.at[i])

    def wrows(own):
        return pl.ds(al((c if own else 1 - c) * OWN, OWN), OWN)

    def load_w(own):
        r = wrows(own)
        return [pltpu.make_async_copy(w_gate.at[r], dw.at[r, pl.ds(0, HID)], lw.at[3 + 2 * own]),
                pltpu.make_async_copy(w_up.at[r], dw.at[r, pl.ds(HID, HID)], lw.at[4 + 2 * own])]

    def start(copies):
        for l in copies:
            l.start()

    def wait(copies):
        for l in copies:
            l.wait()

    def rc(src, dst, kind, sem, dev, slot=0):
        return pltpu.make_async_remote_copy(src, dst, send.at[7 + slot if kind == D2D else kind], sem,
                                            device_id=dev, device_id_type=MESH)

    def cols(h):
        return pl.ds(al(c * OWN + h * HC, HC), HC)

    def cp(k, kind, h, first_chunk=False):
        sem = fin.at[kind - FIN1] if kind >= FIN1 else recv.at[C if first_chunk and h else k, kind]
        if kind == D2D:
            return rc(d2d_s.at[k % SS, h], d2d_r.at[k, h], kind, sem, partner, k % SS)
        if kind == RS1:
            return rc(rs1_s.at[k, h], rs1_r.at[k, h], kind, sem, to_first[h])
        if kind == RS2:
            return rc(rs2_s.at[k, h], rs2_r.at[k, h], kind, sem, to_second[h])
        if kind == AG1:
            b = dx.at[pl.ds(al(k * R + first[h] * R2 + second[h] * R4, R4), R4), cols(h)]
            return rc(b, b, kind, sem, to_second[h])
        p = (1 - first[h]) if kind == FIN2 else first[h]
        b = dx.at[pl.ds(al(k * R + p * R2, R2), R2), cols(h)]
        return rc(b, b, kind, sem, to_first[h] if kind == AG2 else partner)

    def go(k, kind):
        for h in both:
            cp(k, kind, h).start()

    sizes = {D2D: d2d_r, RS1: rs1_r, RS2: rs2_r, AG1: rs2_r, AG2: rs1_r, FIN1: rs1_r, FIN2: rs1_r}

    def sent(slot):
        rc(d2d_s.at[slot], d2d_r.at[0], D2D, fin.at[0], partner, slot).wait_send()

    def arrived(k, kind):
        b = sizes[kind].at[k]
        rc(b, b, kind, recv.at[k, kind], partner).wait_recv()

    stage = (st0, st1)

    def hidden(k, slot):
        r = pl.ds(al(k * R, R), R)
        st = stage[slot]
        dh = dot(dyv[r, :], dwd[...], NT)
        for i in range(3):
            n = slice(i * 256, (i + 1) * 256)
            g, u, d = gv[slot, :, n].astype(F32), uv[slot, :, n].astype(F32), dh[:, n]
            s = jax.nn.sigmoid(g)
            silu = g * s
            hid[r, n] = (silu * u).astype(BF)
            m = slice(HID + i * 256, HID + (i + 1) * 256)
            d_up = (d * silu).astype(BF)
            d_gate = (d * u * (s + silu * (1.0 - s))).astype(BF)
            st[:, m], dgu[r, m] = d_up, d_up
            st[:, n], dgu[r, n] = d_gate, d_gate

    def term(k, slot, own, halves=both):
        n = HC * len(halves)
        w = pl.ds(al((c if own else 1 - c) * OWN + halves[0] * HC, HC), n)
        t = dot(stage[slot][...], dw[w, :], NT)
        for h in halves:
            part = t[:, (h - halves[0]) * HC:(h - halves[0] + 1) * HC]
            if own:
                acc1[slot, h] = part
            else:
                d2d_s[slot, h] = part.astype(BF)

    def add1(k, h):
        keep, leave = (pl.ds(al(v * R2, R2), R2) for v in (first[h], 1 - first[h]))
        rs1_s[k, h] = (acc1[k % S1, h, leave] + d2d_r[k, h, leave].astype(F32)).astype(BF)
        acc2[k % S2, h] = acc1[k % S1, h, keep] + d2d_r[k, h, keep].astype(F32)

    def sum1(k):
        arrived(k, D2D)
        for h in both:
            add1(k, h)
        go(k, RS1)

    def sum2(k):
        arrived(k, RS1)
        for h in both:
            keep, leave = (pl.ds(al(v * R4, R4), R4) for v in (second[h], 1 - second[h]))
            rs2_s[k, h] = (acc2[k % S2, h, leave] + rs1_r[k, h, leave].astype(F32)).astype(BF)
            acc3[k % S3, h] = acc2[k % S2, h, keep] + rs1_r[k, h, keep].astype(F32)
        go(k, RS2)

    def sum3(k):
        arrived(k, RS2)
        for h in both:
            p = first[h] * R2 + second[h] * R4
            dx[pl.ds(al(k * R + p, R4), R4), cols(h)] = (acc3[k % S3, h] + rs2_r[k, h].astype(F32)).astype(BF)
        go(k, AG1)

    def gather2(k):
        arrived(k, AG1)
        go(k, AG2)
        go(k, FIN1)

    def gather3(k):
        arrived(k, AG2)
        go(k, FIN2)

    barrier = pltpu.get_barrier_semaphore()
    for dev in (partner, ny, nx):
        pl.semaphore_signal(barrier, inc=1, device_id=dev, device_id_type=MESH)

    k0 = i32(0)
    chunk0 = load_chunk(k0)
    for i in range(3):
        load_down(i).start()
        chunk0[i].start()
    start(load_w(0))
    start(load_w(1))
    start(load_chunk(i32(1)))
    for i in range(3):
        load_down(i).wait()
    wait(chunk0)
    hidden(k0, 0)
    wait(load_w(0))
    pl.semaphore_wait(barrier, 3)
    term(k0, 0, 0)
    for h in both:
        cp(k0, D2D, h, True).start()
    wait(load_w(1))
    wait(load_chunk(i32(1)))
    start(load_chunk(i32(2)))
    hidden(i32(1), 1)
    term(k0, 0, 1)
    for h in both:
        cp(k0, D2D, h, True).wait_recv()
        add1(k0, h)
        cp(k0, RS1, h).start()
    for j in range(XS):
        load_x(j).start()

    def step(k, slot, last=False):
        if not last:
            @pl.when(k + 2 < C)
            def _():
                start(load_chunk(k + 2))

        @pl.when(k >= 2)
        def _():
            sum1(k - 1)

        @pl.when(k >= 4)
        def _():
            sum2(k - 3)

        @pl.when(k >= 5)
        def _():
            sum3(k - 5)

        @pl.when(k >= 2)
        def _():
            sent(slot)

        for h in both:
            term(k, slot, 0, (h,))
            cp(k, D2D, h).start()
        if slot == 0:
            @pl.when(k == 2)
            def _():
                sum2(i32(0))

        if not last:
            wait(load_chunk(k + 1))
            hidden(k + 1, 1 - slot)
        term(k, slot, 1)

    @pl.loop(0, C // 2 - 1)
    def _(i):
        step(2 * i + 1, 1)
        step(2 * i + 2, 0)

    step(i32(C - 1), 1, last=True)

    def piece_x(j):
        load_x(j).wait()
        dw[j * XB:(j + 1) * XB, :] = dot(xv[j % XS], dgu[...], TN).astype(BF)
        if j + XS < D // XB:
            load_x(j + XS).start()

    def piece_y(j):
        n = slice(j * DB, (j + 1) * DB)
        dwd[:, n] = dot(hid[...], dyv[:, n], TN).astype(BF)

    pieces = []
    for j in range(4):
        pieces += [lambda j=j: piece_x(2 * j), lambda j=j: piece_x(2 * j + 1), lambda j=j: piece_y(j)]
    events = {
        0: [(sum1, 7)],
        1: [(sum2, 5)],
        2: [(sum3, 3)],
        3: [(sum2, 6)],
        4: [(sum3, 4), (gather2, 0)],
        5: [(gather2, 1)],
        6: [(sum2, 7), (gather2, 2)],
        7: [(sum3, 5)],
        8: [(sum3, 6), (gather2, 3)],
        9: [(gather2, 4), (gather3, 0)],
        10: [(sum3, 7)],
        11: [(gather2, 5), (gather3, 1)],
    }
    for i, piece in enumerate(pieces):
        for f, k in events[i]:
            f(i32(k))
        piece()
    for f, k in [(gather2, 6), (gather3, 2), (gather3, 3), (gather3, 4), (gather2, 7), (gather3, 5), (gather3, 6), (gather3, 7)]:
        f(i32(k))

    for kind, b in sizes.items():
        w = rc(b, b, kind, fin.at[max(kind - FIN1, 0)], partner)
        if kind >= FIN1:
            w.wait_recv()
        if kind != D2D:
            w.wait_send()
    for slot in range(SS):
        sent(slot)


def put(dx, dw, dwd, o_dx, o_gate, o_up, o_down, sem):
    copies = []

    def add(a, b):
        copies.append(pltpu.make_async_copy(a, b, sem.at[len(copies)]))

    for i in range(4):
        n = ROWS // 4
        r = pl.ds(i * n, n)
        add(dx.at[r], o_dx.at[r])
        add(dw.at[r, pl.ds(0, HID)], o_gate.at[r])
        add(dw.at[r, pl.ds(HID, HID)], o_up.at[r])
        if i < 4:
            n = HID // 4
            r = pl.ds(i * n, n)
            add(dwd.at[r], o_down.at[r])
    for i, c in enumerate(copies):
        c.start(priority=i % 2 if False else 0)
    for c in copies:
        c.wait()


def solution(mesh):
    def step(*args):
        outs = pl.pallas_call(
            kernel,
            out_shape=[pltpu.VMEM((ROWS, D), BF), pltpu.VMEM((D, 2 * HID), BF), pltpu.VMEM((HID, D), BF)],
            in_specs=[pl.BlockSpec(memory_space=pltpu.HBM)] * 7,
            out_specs=[pl.BlockSpec(memory_space=pltpu.VMEM)] * 3,
            scratch_shapes=[
                pltpu.VMEM((ROWS, D), BF),
                pltpu.VMEM((2, R, HID), BF),
                pltpu.VMEM((2, R, HID), BF),
                pltpu.VMEM((ROWS, 2 * HID), BF),
                pltpu.VMEM((ROWS, HID), BF),
                pltpu.VMEM((R, 2 * HID), BF),
                pltpu.VMEM((R, 2 * HID), BF),
                pltpu.VMEM((XS, ROWS, XB), BF),
                pltpu.VMEM((S1, 2, R, HC), F32),
                pltpu.VMEM((S2, 2, R2, HC), F32),
                pltpu.VMEM((S3, 2, R4, HC), F32),
                pltpu.VMEM((SS, 2, R, HC), BF),
                pltpu.VMEM((C, 2, R, HC), BF),
                pltpu.VMEM((C, 2, R2, HC), BF),
                pltpu.VMEM((C, 2, R2, HC), BF),
                pltpu.VMEM((C, 2, R4, HC), BF),
                pltpu.VMEM((C, 2, R4, HC), BF),
                pltpu.SemaphoreType.DMA((7 + SS,)),
                pltpu.SemaphoreType.DMA((C + 1, 5)),
                pltpu.SemaphoreType.DMA((2,)),
                pltpu.SemaphoreType.DMA((7,)),
                pltpu.SemaphoreType.DMA((2, 3)),
                pltpu.SemaphoreType.DMA((XS,)),
            ],
            compiler_params=pltpu.CompilerParams(collective_id=0, has_side_effects=True, vmem_limit_bytes=46 * 2**20),
        )(*args)
        shapes = [(ROWS, D), (D, HID), (D, HID), (HID, D)]
        return tuple(pl.pallas_call(
            put,
            out_shape=[pltpu.HBM(s, BF) for s in shapes],
            in_specs=[pl.BlockSpec(memory_space=pltpu.VMEM)] * 3,
            out_specs=[pl.BlockSpec(memory_space=pltpu.HBM)] * 4,
            scratch_shapes=[pltpu.SemaphoreType.DMA((16,))],
            compiler_params=pltpu.CompilerParams(vmem_limit_bytes=2**20),
        )(*outs))

    tokens, columns, rows = P("dp", None), P(None, "tp"), P("tp", None)
    return jax.shard_map(
        step,
        mesh=mesh,
        in_specs=(tokens, tokens, P("dp", "tp"), P("dp", "tp"), columns, columns, rows),
        out_specs=(tokens, P("dp", "tp"), P("dp", "tp"), P(("dp", "tp"), None)),
        check_vma=False,
    )
```

```python
import jax
import jax.numpy as jnp
from jax import lax
from jax.experimental import pallas as pl
from jax.experimental.pallas import tpu as pltpu
from jax.sharding import PartitionSpec as P

MESH = pl.DeviceIdType.MESH
BF, F32 = jnp.bfloat16, jnp.float32
NT = (((1,), (1,)), ((), ()))
TN = (((0,), (0,)), ((), ()))

ROWS, D, HID = 2048, 2048, 768
R = 256
C = ROWS // R
R2, R4 = R // 2, R // 4
OWN = D // 2
HC = OWN // 2
XB = 256
DB = 512
SS, XS, S1, S2, S3 = 2, 3, 2, 3, 3

D2D, RS1, RS2, AG1, AG2, FIN1, FIN2 = range(7)


def dot(a, b, dims):
    return lax.dot_general(a, b, dims, preferred_element_type=F32)


def al(v, m):
    return pl.multiple_of(v, m)


def kernel(x, dy, gate, up, w_gate, w_up, w_down, dx, dw, dwd,
           dyv, gv, uv, dgu, hid, st0, st1, xv, acc1, acc2, acc3, d2d_s, d2d_r, rs1_s, rs1_r, rs2_s, rs2_r,
           send, recv, fin, lw, lc, lx):
    me = lax.axis_index("tp")
    c, y, xx = me % 2, (me // 2) % 2, me // 4
    partner = {"tp": me + 1 - 2 * c}
    ny = {"tp": me + 2 - 4 * y}
    nx = {"tp": me + 4 - 8 * xx}
    first, second = (xx, y), (y, xx)
    to_first, to_second = (nx, ny), (ny, nx)
    both = (0, 1)
    i32 = jnp.int32

    def load_chunk(k):
        slot = k % 2
        r = pl.ds(al(k * R, R), R)
        return [pltpu.make_async_copy(dy.at[r], dyv.at[r], lc.at[slot, 0]),
                pltpu.make_async_copy(gate.at[r], gv.at[slot], lc.at[slot, 1]),
                pltpu.make_async_copy(up.at[r], uv.at[slot], lc.at[slot, 2])]

    def load_x(j):
        slot = j % XS
        return pltpu.make_async_copy(x.at[:, pl.ds(j * XB, XB)], xv.at[slot], lx.at[slot])

    def load_half(i):
        n, r = pl.ds(i * OWN, OWN), pl.ds(0, R)
        return [pltpu.make_async_copy(dy.at[r, n], dyv.at[r, n], lw.at[i]),
                pltpu.make_async_copy(w_down.at[:, n], dwd.at[:, n], lw.at[7 + i])]

    def wrows(own):
        return pl.ds(al((c if own else 1 - c) * OWN, OWN), OWN)

    def load_w(own):
        r = wrows(own)
        return [pltpu.make_async_copy(w_gate.at[r], dw.at[r, pl.ds(0, HID)], lw.at[3 + 2 * own]),
                pltpu.make_async_copy(w_up.at[r], dw.at[r, pl.ds(HID, HID)], lw.at[4 + 2 * own])]

    def start(copies):
        for l in copies:
            l.start()

    def wait(copies):
        for l in copies:
            l.wait()

    def rc(src, dst, kind, sem, dev, slot=0):
        return pltpu.make_async_remote_copy(src, dst, send.at[7 + slot if kind == D2D else kind], sem,
                                            device_id=dev, device_id_type=MESH)

    def cols(h):
        return pl.ds(al(c * OWN + h * HC, HC), HC)

    def cp(k, kind, h, first_chunk=False):
        sem = fin.at[kind - FIN1] if kind >= FIN1 else recv.at[C if first_chunk and h else k, kind]
        if kind == D2D:
            return rc(d2d_s.at[k % SS, h], d2d_r.at[k, h], kind, sem, partner, k % SS)
        if kind == RS1:
            return rc(rs1_s.at[k, h], rs1_r.at[k, h], kind, sem, to_first[h])
        if kind == RS2:
            return rc(rs2_s.at[k, h], rs2_r.at[k, h], kind, sem, to_second[h])
        if kind == AG1:
            b = dx.at[pl.ds(al(k * R + first[h] * R2 + second[h] * R4, R4), R4), cols(h)]
            return rc(b, b, kind, sem, to_second[h])
        p = (1 - first[h]) if kind == FIN2 else first[h]
        b = dx.at[pl.ds(al(k * R + p * R2, R2), R2), cols(h)]
        return rc(b, b, kind, sem, to_first[h] if kind == AG2 else partner)

    def go(k, kind):
        for h in both:
            cp(k, kind, h).start()

    sizes = {D2D: d2d_r, RS1: rs1_r, RS2: rs2_r, AG1: rs2_r, AG2: rs1_r, FIN1: rs1_r, FIN2: rs1_r}

    def sent(slot):
        rc(d2d_s.at[slot], d2d_r.at[0], D2D, fin.at[0], partner, slot).wait_send()

    def arrived(k, kind):
        b = sizes[kind].at[k]
        rc(b, b, kind, recv.at[k, kind], partner).wait_recv()

    stage = (st0, st1)

    def hidden(k, slot):
        hidden2(k, slot, dot(dyv[pl.ds(al(k * R, R), R), :], dwd[...], NT))

    def hidden2(k, slot, dh):
        r = pl.ds(al(k * R, R), R)
        st = stage[slot]
        for i in range(3):
            n = slice(i * 256, (i + 1) * 256)
            g, u, d = gv[slot, :, n].astype(F32), uv[slot, :, n].astype(F32), dh[:, n]
            s = jax.nn.sigmoid(g)
            silu = g * s
            hid[r, n] = (silu * u).astype(BF)
            m = slice(HID + i * 256, HID + (i + 1) * 256)
            d_up = (d * silu).astype(BF)
            d_gate = (d * u * (s + silu * (1.0 - s))).astype(BF)
            st[:, m], dgu[r, m] = d_up, d_up
            st[:, n], dgu[r, n] = d_gate, d_gate

    def term(k, slot, own, halves=both):
        n = HC * len(halves)
        w = pl.ds(al((c if own else 1 - c) * OWN + halves[0] * HC, HC), n)
        t = dot(stage[slot][...], dw[w, :], NT)
        for h in halves:
            part = t[:, (h - halves[0]) * HC:(h - halves[0] + 1) * HC]
            if own:
                acc1[slot, h] = part
            else:
                d2d_s[slot, h] = part.astype(BF)

    def add1(k, h):
        keep, leave = (pl.ds(al(v * R2, R2), R2) for v in (first[h], 1 - first[h]))
        rs1_s[k, h] = (acc1[k % S1, h, leave] + d2d_r[k, h, leave].astype(F32)).astype(BF)
        acc2[k % S2, h] = acc1[k % S1, h, keep] + d2d_r[k, h, keep].astype(F32)

    def sum1(k):
        arrived(k, D2D)
        for h in both:
            add1(k, h)
        go(k, RS1)

    def sum2(k):
        arrived(k, RS1)
        for h in both:
            keep, leave = (pl.ds(al(v * R4, R4), R4) for v in (second[h], 1 - second[h]))
            rs2_s[k, h] = (acc2[k % S2, h, leave] + rs1_r[k, h, leave].astype(F32)).astype(BF)
            acc3[k % S3, h] = acc2[k % S2, h, keep] + rs1_r[k, h, keep].astype(F32)
        go(k, RS2)

    def sum3(k):
        arrived(k, RS2)
        for h in both:
            p = first[h] * R2 + second[h] * R4
            dx[pl.ds(al(k * R + p, R4), R4), cols(h)] = (acc3[k % S3, h] + rs2_r[k, h].astype(F32)).astype(BF)
        go(k, AG1)

    def gather2(k):
        arrived(k, AG1)
        go(k, AG2)
        go(k, FIN1)

    def gather3(k):
        arrived(k, AG2)
        go(k, FIN2)

    barrier = pltpu.get_barrier_semaphore()
    for dev in (partner, ny, nx):
        pl.semaphore_signal(barrier, inc=1, device_id=dev, device_id_type=MESH)

    k0 = i32(0)
    chunk0 = load_chunk(k0)[1:]
    start(load_half(0))
    start(load_half(1))
    start(chunk0)
    start(load_w(0))
    start(load_w(1))
    start(load_chunk(i32(1)))
    wait(load_half(0))
    left = dot(dyv[:R, :OWN], dwd[:, :OWN], NT)
    acc1[1, 0] = left[:, :HC]
    acc1[1, 1, :, :HID - HC] = left[:, HC:]
    wait(load_half(1))
    wait(chunk0)
    left = jnp.concatenate([acc1[1, 0], acc1[1, 1, :, :HID - HC]], axis=1)
    hidden2(k0, 0, left + dot(dyv[:R, OWN:], dwd[:, OWN:], NT))
    wait(load_w(0))
    pl.semaphore_wait(barrier, 3)
    term(k0, 0, 0)
    for h in both:
        cp(k0, D2D, h, True).start()
    wait(load_w(1))
    wait(load_chunk(i32(1)))
    start(load_chunk(i32(2)))
    hidden(i32(1), 1)
    term(k0, 0, 1)
    for h in both:
        cp(k0, D2D, h, True).wait_recv()
        add1(k0, h)
        cp(k0, RS1, h).start()
    for j in range(XS):
        load_x(j).start()

    def step(k, slot, last=False):
        if not last:
            @pl.when(k + 2 < C)
            def _():
                start(load_chunk(k + 2))

        @pl.when(k >= 2)
        def _():
            sum1(k - 1)

        @pl.when(k >= 4)
        def _():
            sum2(k - 3)

        @pl.when(k >= 5)
        def _():
            sum3(k - 5)

        @pl.when(k >= 2)
        def _():
            sent(slot)

        for h in both:
            term(k, slot, 0, (h,))
            cp(k, D2D, h).start()
        if slot == 0:
            @pl.when(k == 2)
            def _():
                sum2(i32(0))

        if not last:
            wait(load_chunk(k + 1))
            hidden(k + 1, 1 - slot)
        term(k, slot, 1)

    @pl.loop(0, C // 2 - 1)
    def _(i):
        step(2 * i + 1, 1)
        step(2 * i + 2, 0)

    step(i32(C - 1), 1, last=True)

    def piece_x(j):
        load_x(j).wait()
        dw[j * XB:(j + 1) * XB, :] = dot(xv[j % XS], dgu[...], TN).astype(BF)
        if j + XS < D // XB:
            load_x(j + XS).start()

    def piece_y(j):
        n = slice(j * DB, (j + 1) * DB)
        dwd[:, n] = dot(hid[...], dyv[:, n], TN).astype(BF)

    pieces = []
    for j in range(4):
        pieces += [lambda j=j: piece_x(2 * j), lambda j=j: piece_x(2 * j + 1), lambda j=j: piece_y(j)]
    events = {
        0: [(sum1, 7)],
        1: [(sum2, 5)],
        2: [(sum3, 3)],
        3: [(sum2, 6)],
        4: [(sum3, 4), (gather2, 0)],
        5: [(gather2, 1)],
        6: [(sum2, 7), (gather2, 2)],
        7: [(sum3, 5)],
        8: [(sum3, 6), (gather2, 3)],
        9: [(gather2, 4), (gather3, 0)],
        10: [(sum3, 7)],
        11: [(gather2, 5), (gather3, 1)],
    }
    for i, piece in enumerate(pieces):
        for f, k in events[i]:
            f(i32(k))
        piece()
    for f, k in [(gather2, 6), (gather3, 2), (gather3, 3), (gather3, 4), (gather2, 7), (gather3, 5), (gather3, 6), (gather3, 7)]:
        f(i32(k))

    for kind, b in sizes.items():
        w = rc(b, b, kind, fin.at[max(kind - FIN1, 0)], partner)
        if kind >= FIN1:
            w.wait_recv()
        if kind != D2D:
            w.wait_send()
    for slot in range(SS):
        sent(slot)


def put(dx, dw, dwd, o_dx, o_gate, o_up, o_down, sem):
    copies = []

    def add(a, b):
        copies.append(pltpu.make_async_copy(a, b, sem.at[len(copies)]))

    for i in range(4):
        n = ROWS // 4
        r = pl.ds(i * n, n)
        add(dx.at[r], o_dx.at[r])
        add(dw.at[r, pl.ds(0, HID)], o_gate.at[r])
        add(dw.at[r, pl.ds(HID, HID)], o_up.at[r])
        if i < 4:
            n = HID // 4
            r = pl.ds(i * n, n)
            add(dwd.at[r], o_down.at[r])
    for i, c in enumerate(copies):
        c.start(priority=i % 2 if False else 0)
    for c in copies:
        c.wait()


def solution(mesh):
    def step(*args):
        outs = pl.pallas_call(
            kernel,
            out_shape=[pltpu.VMEM((ROWS, D), BF), pltpu.VMEM((D, 2 * HID), BF), pltpu.VMEM((HID, D), BF)],
            in_specs=[pl.BlockSpec(memory_space=pltpu.HBM)] * 7,
            out_specs=[pl.BlockSpec(memory_space=pltpu.VMEM)] * 3,
            scratch_shapes=[
                pltpu.VMEM((ROWS, D), BF),
                pltpu.VMEM((2, R, HID), BF),
                pltpu.VMEM((2, R, HID), BF),
                pltpu.VMEM((ROWS, 2 * HID), BF),
                pltpu.VMEM((ROWS, HID), BF),
                pltpu.VMEM((R, 2 * HID), BF),
                pltpu.VMEM((R, 2 * HID), BF),
                pltpu.VMEM((XS, ROWS, XB), BF),
                pltpu.VMEM((S1, 2, R, HC), F32),
                pltpu.VMEM((S2, 2, R2, HC), F32),
                pltpu.VMEM((S3, 2, R4, HC), F32),
                pltpu.VMEM((SS, 2, R, HC), BF),
                pltpu.VMEM((C, 2, R, HC), BF),
                pltpu.VMEM((C, 2, R2, HC), BF),
                pltpu.VMEM((C, 2, R2, HC), BF),
                pltpu.VMEM((C, 2, R4, HC), BF),
                pltpu.VMEM((C, 2, R4, HC), BF),
                pltpu.SemaphoreType.DMA((7 + SS,)),
                pltpu.SemaphoreType.DMA((C + 1, 5)),
                pltpu.SemaphoreType.DMA((2,)),
                pltpu.SemaphoreType.DMA((9,)),
                pltpu.SemaphoreType.DMA((2, 3)),
                pltpu.SemaphoreType.DMA((XS,)),
            ],
            compiler_params=pltpu.CompilerParams(collective_id=0, has_side_effects=True, vmem_limit_bytes=46 * 2**20),
        )(*args)
        shapes = [(ROWS, D), (D, HID), (D, HID), (HID, D)]
        return tuple(pl.pallas_call(
            put,
            out_shape=[pltpu.HBM(s, BF) for s in shapes],
            in_specs=[pl.BlockSpec(memory_space=pltpu.VMEM)] * 3,
            out_specs=[pl.BlockSpec(memory_space=pltpu.HBM)] * 4,
            scratch_shapes=[pltpu.SemaphoreType.DMA((16,))],
            compiler_params=pltpu.CompilerParams(vmem_limit_bytes=2**20),
        )(*outs))

    tokens, columns, rows = P("dp", None), P(None, "tp"), P("tp", None)
    return jax.shard_map(
        step,
        mesh=mesh,
        in_specs=(tokens, tokens, P("dp", "tp"), P("dp", "tp"), columns, columns, rows),
        out_specs=(tokens, P("dp", "tp"), P("dp", "tp"), P(("dp", "tp"), None)),
        check_vma=False,
    )
```

```python
import jax
import jax.numpy as jnp
from jax import lax
from jax.experimental import pallas as pl
from jax.experimental.pallas import tpu as pltpu
from jax.sharding import PartitionSpec as P

MESH = pl.DeviceIdType.MESH
BF, F32 = jnp.bfloat16, jnp.float32
NT = (((1,), (1,)), ((), ()))
TN = (((0,), (0,)), ((), ()))

ROWS, D, HID = 2048, 2048, 768
R = 256
C = ROWS // R
R2, R4 = R // 2, R // 4
OWN = D // 2
HC = OWN // 2
XB = 256
DB = 512
RT = 16
SS, XS, S1, S2, S3 = 2, 3, 2, 3, 3

D2D, RS1, RS2, AG1, AG2, FIN1, FIN2 = range(7)


def dot(a, b, dims):
    return lax.dot_general(a, b, dims, preferred_element_type=F32)


def al(v, m):
    return pl.multiple_of(v, m)


def kernel(x, dy, gate, up, w_gate, w_up, w_down, dx, dw, dwd,
           dyv, gv, uv, dgu, hid, st0, st1, xv, acc1, acc2, acc3, d2d_s, d2d_r, rs1_s, rs1_r, rs2_s, rs2_r,
           send, recv, fin, last, lw, lc, lx):
    me = lax.axis_index("tp")
    c, y, xx = me % 2, (me // 2) % 2, me // 4
    partner = {"tp": me + 1 - 2 * c}
    ny = {"tp": me + 2 - 4 * y}
    nx = {"tp": me + 4 - 8 * xx}
    first, second = (xx, y), (y, xx)
    to_first, to_second = (nx, ny), (ny, nx)
    to_other = tuple({"tp": d["tp"] + 1 - 2 * c} for d in to_first)
    both = (0, 1)
    i32 = jnp.int32

    def load_chunk(k):
        slot = k % 2
        r = pl.ds(al(k * R, R), R)
        return [pltpu.make_async_copy(dy.at[r], dyv.at[r], lc.at[slot, 0]),
                pltpu.make_async_copy(gate.at[r], gv.at[slot], lc.at[slot, 1]),
                pltpu.make_async_copy(up.at[r], uv.at[slot], lc.at[slot, 2])]

    def load_x(j):
        slot = j % XS
        return pltpu.make_async_copy(x.at[:, pl.ds(j * XB, XB)], xv.at[slot], lx.at[slot])

    def load_half(i):
        n, r = pl.ds(i * OWN, OWN), pl.ds(0, R)
        return [pltpu.make_async_copy(dy.at[r, n], dyv.at[r, n], lw.at[i]),
                pltpu.make_async_copy(w_down.at[:, n], dwd.at[:, n], lw.at[7 + i])]

    def wrows(own):
        return pl.ds(al((c if own else 1 - c) * OWN, OWN), OWN)

    def load_w(own):
        r = wrows(own)
        return [pltpu.make_async_copy(w_gate.at[r], dw.at[r, pl.ds(0, HID)], lw.at[3 + 2 * own]),
                pltpu.make_async_copy(w_up.at[r], dw.at[r, pl.ds(HID, HID)], lw.at[4 + 2 * own])]

    def start(copies):
        for l in copies:
            l.start()

    def wait(copies):
        for l in copies:
            l.wait()

    def rc(src, dst, kind, sem, dev, slot=0):
        return pltpu.make_async_remote_copy(src, dst, send.at[7 + slot if kind == D2D else kind], sem,
                                            device_id=dev, device_id_type=MESH)

    def cols(h):
        return pl.ds(al(c * OWN + h * HC, HC), HC)

    def cp(k, kind, h, first_chunk=False):
        sem = fin.at[kind - FIN1] if kind >= FIN1 else recv.at[C if first_chunk and h else k, kind]
        if kind == D2D:
            return rc(d2d_s.at[k % SS, h], d2d_r.at[k, h], kind, sem, partner, k % SS)
        if kind == RS1:
            return rc(rs1_s.at[k, h], rs1_r.at[k, h], kind, sem, to_first[h])
        if kind == RS2:
            return rc(rs2_s.at[k, h], rs2_r.at[k, h], kind, sem, to_second[h])
        if kind == AG1:
            b = dx.at[pl.ds(al(k * R + first[h] * R2 + second[h] * R4, R4), R4), cols(h)]
            return rc(b, b, kind, sem, to_second[h])
        p = (1 - first[h]) if kind == FIN2 else first[h]
        b = dx.at[pl.ds(al(k * R + p * R2, R2), R2), cols(h)]
        return rc(b, b, kind, sem, to_first[h] if kind == AG2 else partner)

    def go(k, kind):
        for h in both:
            cp(k, kind, h).start()

    sizes = {D2D: d2d_r, RS1: rs1_r, RS2: rs2_r, AG1: rs2_r, AG2: rs1_r, FIN1: rs1_r, FIN2: rs1_r}

    def sent(slot):
        rc(d2d_s.at[slot], d2d_r.at[0], D2D, fin.at[0], partner, slot).wait_send()

    def arrived(k, kind):
        b = sizes[kind].at[k]
        rc(b, b, kind, recv.at[k, kind], partner).wait_recv()

    stage = (st0, st1)

    def hidden(k, slot):
        hidden2(k, slot, dot(dyv[pl.ds(al(k * R, R), R), :], dwd[...], NT))

    def hidden2(k, slot, dh):
        r = pl.ds(al(k * R, R), R)
        st = stage[slot]
        for i in range(3):
            n = slice(i * 256, (i + 1) * 256)
            g, u, d = gv[slot, :, n].astype(F32), uv[slot, :, n].astype(F32), dh[:, n]
            s = jax.nn.sigmoid(g)
            silu = g * s
            hid[r, n] = (silu * u).astype(BF)
            m = slice(HID + i * 256, HID + (i + 1) * 256)
            d_up = (d * silu).astype(BF)
            d_gate = (d * u * (s + silu * (1.0 - s))).astype(BF)
            st[:, m], dgu[r, m] = d_up, d_up
            st[:, n], dgu[r, n] = d_gate, d_gate

    def term(k, slot, own, halves=both):
        n = HC * len(halves)
        w = pl.ds(al((c if own else 1 - c) * OWN + halves[0] * HC, HC), n)
        t = dot(stage[slot][...], dw[w, :], NT)
        for h in halves:
            part = t[:, (h - halves[0]) * HC:(h - halves[0] + 1) * HC]
            if own:
                acc1[slot, h] = part
            else:
                d2d_s[slot, h] = part.astype(BF)

    def add1(k, h):
        keep, leave = (pl.ds(al(v * R2, R2), R2) for v in (first[h], 1 - first[h]))
        rs1_s[k, h] = (acc1[k % S1, h, leave] + d2d_r[k, h, leave].astype(F32)).astype(BF)
        acc2[k % S2, h] = acc1[k % S1, h, keep] + d2d_r[k, h, keep].astype(F32)

    def sum1(k):
        arrived(k, D2D)
        for h in both:
            add1(k, h)
        go(k, RS1)

    def sum2(k):
        arrived(k, RS1)
        for h in both:
            keep, leave = (pl.ds(al(v * R4, R4), R4) for v in (second[h], 1 - second[h]))
            rs2_s[k, h] = (acc2[k % S2, h, leave] + rs1_r[k, h, leave].astype(F32)).astype(BF)
            acc3[k % S3, h] = acc2[k % S2, h, keep] + rs1_r[k, h, keep].astype(F32)
        go(k, RS2)

    def sum3(k):
        arrived(k, RS2)
        for h in both:
            p = first[h] * R2 + second[h] * R4
            dx[pl.ds(al(k * R + p, R4), R4), cols(h)] = (acc3[k % S3, h] + rs2_r[k, h].astype(F32)).astype(BF)
        go(k, AG1)

    def gather2(k):
        arrived(k, AG1)
        go(k, AG2)
        go(k, FIN1)

    def gather3(k):
        arrived(k, AG2)
        go(k, FIN2)

    kl = C - 1

    def lastcp(kind, h, tail, sem, dev):
        p = ((1 - first[h]) if kind == FIN2 else first[h]) * R2 + (R2 - RT if tail else 0)
        b = dx.at[pl.ds(al(kl * R + p, RT), RT if tail else R2 - RT), cols(h)]
        return rc(b, b, kind, sem, dev)

    def count(rows, kind, sem):
        b = dx.at[pl.ds(0, rows), pl.ds(0, OWN)]
        return rc(b, b, kind, sem, partner)

    def last2():
        arrived(kl, AG1)
        for tail in (False, True):
            for h in both:
                lastcp(AG2, h, tail, last.at[0] if tail else recv.at[kl, AG2], to_first[h]).start()
                if tail:
                    lastcp(AG2, h, tail, last.at[0], to_other[h]).start()
        go(kl, FIN1)

    def last3():
        count(R2 - RT, AG2, recv.at[kl, AG2]).wait_recv()
        for h in both:
            lastcp(FIN2, h, False, fin.at[1], partner).start()
        count(2 * RT, AG2, last.at[0]).wait_recv()

    barrier = pltpu.get_barrier_semaphore()
    for dev in (partner, ny, nx, *to_other):
        pl.semaphore_signal(barrier, inc=1, device_id=dev, device_id_type=MESH)

    k0 = i32(0)
    chunk0 = load_chunk(k0)[1:]
    start(load_half(0))
    start(load_half(1))
    start(chunk0)
    start(load_w(0))
    start(load_w(1))
    start(load_chunk(i32(1)))
    wait(load_half(0))
    left = dot(dyv[:R, :OWN], dwd[:, :OWN], NT)
    acc1[1, 0] = left[:, :HC]
    acc1[1, 1, :, :HID - HC] = left[:, HC:]
    wait(load_half(1))
    wait(chunk0)
    left = jnp.concatenate([acc1[1, 0], acc1[1, 1, :, :HID - HC]], axis=1)
    hidden2(k0, 0, left + dot(dyv[:R, OWN:], dwd[:, OWN:], NT))
    wait(load_w(0))
    pl.semaphore_wait(barrier, 5)
    term(k0, 0, 0)
    for h in both:
        cp(k0, D2D, h, True).start()
    wait(load_w(1))
    wait(load_chunk(i32(1)))
    start(load_chunk(i32(2)))
    hidden(i32(1), 1)
    term(k0, 0, 1)
    for h in both:
        cp(k0, D2D, h, True).wait_recv()
        add1(k0, h)
        cp(k0, RS1, h).start()
    for j in range(XS):
        load_x(j).start()

    def step(k, slot, last=False):
        if not last:
            @pl.when(k + 2 < C)
            def _():
                start(load_chunk(k + 2))

        @pl.when(k >= 2)
        def _():
            sum1(k - 1)

        @pl.when(k >= 4)
        def _():
            sum2(k - 3)

        @pl.when(k >= 5)
        def _():
            sum3(k - 5)

        @pl.when(k >= 2)
        def _():
            sent(slot)

        for h in both:
            term(k, slot, 0, (h,))
            cp(k, D2D, h).start()
        if slot == 0:
            @pl.when(k == 2)
            def _():
                sum2(i32(0))

        if not last:
            wait(load_chunk(k + 1))
            hidden(k + 1, 1 - slot)
        term(k, slot, 1)

    @pl.loop(0, C // 2 - 1)
    def _(i):
        step(2 * i + 1, 1)
        step(2 * i + 2, 0)

    step(i32(C - 1), 1, last=True)

    def piece_x(j):
        load_x(j).wait()
        dw[j * XB:(j + 1) * XB, :] = dot(xv[j % XS], dgu[...], TN).astype(BF)
        if j + XS < D // XB:
            load_x(j + XS).start()

    def piece_y(j):
        n = slice(j * DB, (j + 1) * DB)
        dwd[:, n] = dot(hid[...], dyv[:, n], TN).astype(BF)

    pieces = []
    for j in range(4):
        pieces += [lambda j=j: piece_x(2 * j), lambda j=j: piece_x(2 * j + 1), lambda j=j: piece_y(j)]
    events = {
        0: [(sum1, 7)],
        1: [(sum2, 5)],
        2: [(sum3, 3)],
        3: [(sum2, 6)],
        4: [(sum3, 4), (gather2, 0)],
        5: [(gather2, 1)],
        6: [(sum2, 7), (gather2, 2)],
        7: [(sum3, 5)],
        8: [(sum3, 6), (gather2, 3)],
        9: [(gather2, 4), (gather3, 0)],
        10: [(sum3, 7)],
        11: [(gather2, 5), (gather3, 1)],
    }
    for i, piece in enumerate(pieces):
        for f, k in events[i]:
            f(i32(k))
        piece()
    gather2(i32(6))
    for k in (2, 3, 4):
        gather3(i32(k))
    last2()
    for k in (5, 6):
        gather3(i32(k))
    last3()

    for slot in range(SS):
        sent(slot)
    for kind in (RS1, RS2, AG1, FIN1):
        b = sizes[kind]
        w = rc(b, b, kind, fin.at[0], partner)
        w.wait_send()
        if kind == FIN1:
            w.wait_recv()
    count(C * R2 + RT, AG2, fin.at[0]).wait_send()
    w = count(C * R2 - RT, FIN2, fin.at[1])
    w.wait_send()
    w.wait_recv()


def put(dx, dw, dwd, o_dx, o_gate, o_up, o_down, sem):
    copies = []

    def add(a, b):
        copies.append(pltpu.make_async_copy(a, b, sem.at[len(copies)]))

    for i in range(4):
        n = ROWS // 4
        r = pl.ds(i * n, n)
        add(dx.at[r], o_dx.at[r])
        add(dw.at[r, pl.ds(0, HID)], o_gate.at[r])
        add(dw.at[r, pl.ds(HID, HID)], o_up.at[r])
        if i < 4:
            n = HID // 4
            r = pl.ds(i * n, n)
            add(dwd.at[r], o_down.at[r])
    for i, c in enumerate(copies):
        c.start(priority=i % 2 if False else 0)
    for c in copies:
        c.wait()


def solution(mesh):
    def step(*args):
        outs = pl.pallas_call(
            kernel,
            out_shape=[pltpu.VMEM((ROWS, D), BF), pltpu.VMEM((D, 2 * HID), BF), pltpu.VMEM((HID, D), BF)],
            in_specs=[pl.BlockSpec(memory_space=pltpu.HBM)] * 7,
            out_specs=[pl.BlockSpec(memory_space=pltpu.VMEM)] * 3,
            scratch_shapes=[
                pltpu.VMEM((ROWS, D), BF),
                pltpu.VMEM((2, R, HID), BF),
                pltpu.VMEM((2, R, HID), BF),
                pltpu.VMEM((ROWS, 2 * HID), BF),
                pltpu.VMEM((ROWS, HID), BF),
                pltpu.VMEM((R, 2 * HID), BF),
                pltpu.VMEM((R, 2 * HID), BF),
                pltpu.VMEM((XS, ROWS, XB), BF),
                pltpu.VMEM((S1, 2, R, HC), F32),
                pltpu.VMEM((S2, 2, R2, HC), F32),
                pltpu.VMEM((S3, 2, R4, HC), F32),
                pltpu.VMEM((SS, 2, R, HC), BF),
                pltpu.VMEM((C, 2, R, HC), BF),
                pltpu.VMEM((C, 2, R2, HC), BF),
                pltpu.VMEM((C, 2, R2, HC), BF),
                pltpu.VMEM((C, 2, R4, HC), BF),
                pltpu.VMEM((C, 2, R4, HC), BF),
                pltpu.SemaphoreType.DMA((7 + SS,)),
                pltpu.SemaphoreType.DMA((C + 1, 5)),
                pltpu.SemaphoreType.DMA((2,)),
                pltpu.SemaphoreType.DMA((1,)),
                pltpu.SemaphoreType.DMA((9,)),
                pltpu.SemaphoreType.DMA((2, 3)),
                pltpu.SemaphoreType.DMA((XS,)),
            ],
            compiler_params=pltpu.CompilerParams(collective_id=0, has_side_effects=True, vmem_limit_bytes=46 * 2**20),
        )(*args)
        shapes = [(ROWS, D), (D, HID), (D, HID), (HID, D)]
        return tuple(pl.pallas_call(
            put,
            out_shape=[pltpu.HBM(s, BF) for s in shapes],
            in_specs=[pl.BlockSpec(memory_space=pltpu.VMEM)] * 3,
            out_specs=[pl.BlockSpec(memory_space=pltpu.HBM)] * 4,
            scratch_shapes=[pltpu.SemaphoreType.DMA((16,))],
            compiler_params=pltpu.CompilerParams(vmem_limit_bytes=2**20),
        )(*outs))

    tokens, columns, rows = P("dp", None), P(None, "tp"), P("tp", None)
    return jax.shard_map(
        step,
        mesh=mesh,
        in_specs=(tokens, tokens, P("dp", "tp"), P("dp", "tp"), columns, columns, rows),
        out_specs=(tokens, P("dp", "tp"), P("dp", "tp"), P(("dp", "tp"), None)),
        check_vma=False,
    )
```
